8 devices in a mesh: dp: 1 (over z), kvh: 2 (over y), seq: 4 (over x, core).
Axes of the slice: x: 2, y: 2, z: 1, core: 2. Of those that a mesh axis runs over, the one named last changes fastest.
Arguments:
- x_hidden: bfloat16 [128, 6144], P('dp')
- seq_lens: int32 [128], P('dp')
- k_cache: bfloat16 [128, 2048, 8, 128], P('dp', 'seq', 'kvh')
- v_cache: bfloat16 [128, 2048, 8, 128], P('dp', 'seq', 'kvh')
- w_q: bfloat16 [6144, 48, 128], P(None, ('kvh', 'seq'))
- w_o: bfloat16 [48, 128, 6144], P(('kvh', 'seq'))
Outputs:
- output: bfloat16 [128, 6144], P('dp')
All inputs are finite; a program needn't handle non-finite values.
Results may differ from the reference program's by a relative error of at most 0.00348738.
Values are sent between devices in bfloat16 or wider.
A program may use at most 1 GiB of HBM per device.

```python
import jax
import jax.numpy as jnp
from jax import lax

BATCH_ROWS = 128
SEQ_LEN = 2048
MODEL_DIM = 6144
QUERY_HEADS = 48
KV_HEADS = 8
HEAD_DIM = 128
ROPE_THETA = 500000
TOKEN_SEGMENTS = 64


def rotate_query(q_raw, seq_lens):
    half_dim = HEAD_DIM // 2
    inv_freq = jnp.power(float(ROPE_THETA), -jnp.arange(half_dim, dtype=jnp.float32) * (2.0 / HEAD_DIM))
    angle = (seq_lens - 1).astype(jnp.float32)[:, None] * inv_freq[None, :]
    cosine = jnp.cos(angle)[:, None, :]
    sine = jnp.sin(angle)[:, None, :]
    first = q_raw[..., :half_dim]
    second = q_raw[..., half_dim:]
    return jnp.concatenate([first * cosine - second * sine, second * cosine + first * sine], axis=-1)


def setup_inputs(seed: int = 0, part: int = 0) -> dict:
    base_key = jax.random.key(seed)
    key_list = jax.random.split(base_key, 4)
    part_list = jax.random.split(jax.random.fold_in(key_list[0], part), 8)
    seg_len = SEQ_LEN // TOKEN_SEGMENTS
    low_len = SEQ_LEN // 4
    x_hidden = jax.random.normal(part_list[0], (BATCH_ROWS, MODEL_DIM), jnp.float32).astype(jnp.bfloat16)
    seq_lens = jax.random.randint(part_list[1], (BATCH_ROWS,), low_len, SEQ_LEN + 1)
    seq_lens = seq_lens.at[0].set(SEQ_LEN).at[1].set(low_len)
    seq_lens = jax.random.permutation(part_list[2], seq_lens)
    noise_shape = (BATCH_ROWS, TOKEN_SEGMENTS, seg_len, KV_HEADS, HEAD_DIM)
    mean_shape = (BATCH_ROWS, TOKEN_SEGMENTS, 1, KV_HEADS, HEAD_DIM)
    key_mean = 1.5 * jax.random.normal(part_list[3], mean_shape, jnp.float32)
    key_noise = jax.random.normal(part_list[4], noise_shape, jnp.float32)
    k_cache = (key_noise + key_mean).reshape(BATCH_ROWS, SEQ_LEN, KV_HEADS, HEAD_DIM).astype(jnp.bfloat16)
    value_mean = jax.random.normal(part_list[5], mean_shape, jnp.float32)
    value_noise = 0.7 * jax.random.normal(part_list[6], noise_shape, jnp.float32)
    v_cache = (value_noise + value_mean).reshape(BATCH_ROWS, SEQ_LEN, KV_HEADS, HEAD_DIM).astype(jnp.bfloat16)
    w_q = (jax.random.normal(key_list[1], (MODEL_DIM, QUERY_HEADS, HEAD_DIM), jnp.float32) * MODEL_DIM ** -0.5).astype(jnp.bfloat16)
    w_o = (jax.random.normal(key_list[2], (QUERY_HEADS, HEAD_DIM, MODEL_DIM), jnp.float32) * (QUERY_HEADS * HEAD_DIM) ** -0.5).astype(jnp.bfloat16)
    return dict(x_hidden=x_hidden, seq_lens=seq_lens, k_cache=k_cache, v_cache=v_cache, w_q=w_q, w_o=w_o)


def reference(x_hidden, seq_lens, k_cache, v_cache, w_q, w_o):
    group_size = QUERY_HEADS // KV_HEADS
    q_raw = jnp.einsum('bd,dhk->bhk', x_hidden.astype(jnp.float32), w_q.astype(jnp.float32))
    q_rot = rotate_query(q_raw, seq_lens).astype(jnp.bfloat16)
    q_flat = q_rot.reshape(BATCH_ROWS * KV_HEADS, group_size, HEAD_DIM)
    k_flat = k_cache.transpose(0, 2, 1, 3).reshape(BATCH_ROWS * KV_HEADS, SEQ_LEN, HEAD_DIM)
    v_flat = v_cache.transpose(0, 2, 1, 3).reshape(BATCH_ROWS * KV_HEADS, SEQ_LEN, HEAD_DIM)
    len_flat = jnp.repeat(seq_lens, KV_HEADS)
    positions = jnp.arange(SEQ_LEN)

    def one_head(operands):
        q_head, k_head, v_head, length = operands
        scores = jnp.dot(q_head, k_head.T, preferred_element_type=jnp.float32) * (HEAD_DIM ** -0.5)
        valid_mask = positions[None, :] < length
        scores = jnp.where(valid_mask, scores, -jnp.inf)
        weights = jnp.exp(scores - jnp.max(scores, axis=-1, keepdims=True))
        weight_sum = jnp.sum(weights, axis=-1, keepdims=True)
        attn = jnp.dot(weights.astype(jnp.bfloat16), v_head, preferred_element_type=jnp.float32) / weight_sum
        return attn.astype(jnp.bfloat16)

    attn = lax.map(one_head, (q_flat, k_flat, v_flat, len_flat)).reshape(BATCH_ROWS, QUERY_HEADS, HEAD_DIM)
    y_sum = jnp.einsum('bhk,hkd->bd', attn.astype(jnp.float32), w_o.astype(jnp.float32))
    return (x_hidden.astype(jnp.float32) + y_sum).astype(jnp.bfloat16)
```

```python
import functools

import jax
import jax.numpy as jnp
from jax import lax
from jax.experimental import pallas as pl
from jax.experimental.pallas import tpu as pltpu
from jax.sharding import PartitionSpec as P

ROPE_THETA = 500000.0
HEAD_DIM = 128
NEG = -3.3e38
FLOOR = -3.0e38
LOG2E = 1.4426950408889634
SCALE2 = HEAD_DIM ** -0.5 * LOG2E
SLOTS = 16
UNROLL = 2


def rope_tables(seq_lens):
    half_dim = HEAD_DIM // 2
    inv_freq = jnp.power(ROPE_THETA, -jnp.arange(half_dim, dtype=jnp.float32) * (2.0 / HEAD_DIM))
    angle = (seq_lens - 1).astype(jnp.float32)[:, None] * inv_freq[None, :]
    return jnp.cos(angle), jnp.sin(angle)


def head_lanes(width):
    lane = lax.broadcasted_iota(jnp.int32, (8, width), 1)
    return lane, [lane % 4 == n for n in range(4)]


def pick(masks, parts):
    return jnp.where(masks[0], parts[0], jnp.where(masks[1], parts[1], jnp.where(masks[2], parts[2], parts[3])))


def score_row(q32, k_at, limit, p_at, stat_at):
    tiles = k_at.shape[0] // 512
    zero = jnp.zeros_like(q32)
    q_diag = jnp.concatenate([jnp.concatenate([q32, zero], 1), jnp.concatenate([zero, q32], 1)], 0)
    lane, masks = head_lanes(256)
    scores = []
    for j in range(tiles):
        keys = jnp.concatenate([k_at[pl.ds(512 * j, 256), :], k_at[pl.ds(512 * j + 256, 256), :]], 1)
        s = lax.dot_general(q_diag, keys, (((1,), (1,)), ((), ())), preferred_element_type=jnp.float32)
        for h in range(2):
            mine = pick(masks, [s[32 * h + 8 * n:32 * h + 8 * n + 8] for n in range(4)])
            scores.append(jnp.where(lane < limit - (512 * j + 256 * h), mine, NEG))
    top = functools.reduce(jnp.maximum, scores)
    top = jnp.maximum(top[:, :128], top[:, 128:])
    _, half = head_lanes(128)
    tops = [jnp.maximum(jnp.max(jnp.where(half[n], top, NEG), axis=1, keepdims=True), FLOOR) * SCALE2 for n in range(4)]
    shift = pick(half, tops)
    shift = jnp.concatenate([shift, shift], 1)
    total = None
    for j in range(tiles):
        rows = []
        for h in range(2):
            w = jnp.exp2(scores[2 * j + h] * SCALE2 - shift)
            total = w if total is None else total + w
            rows += [jnp.where(masks[n], w, 0.0) for n in range(4)]
        p_at[j] = jnp.concatenate(rows, 0).astype(jnp.bfloat16)
    total = total[:, :128] + total[:, 128:]
    row = lax.broadcasted_iota(jnp.int32, (8, 128), 0)
    lane128 = lax.broadcasted_iota(jnp.int32, (8, 128), 1)
    diagonal = row == lane128
    for n in range(4):
        sums = jnp.sum(jnp.where(half[n], total, 0.0), axis=1, keepdims=True)
        top_row = jnp.sum(jnp.where(diagonal, tops[n], 0.0), axis=0, keepdims=True)
        sum_row = jnp.sum(jnp.where(diagonal, sums, 0.0), axis=0, keepdims=True)
        stat_at[n] = jnp.where(row == 6, top_row, sum_row)


def value_row(p_at, v_at, stat_at, out_at):
    tiles = v_at.shape[0] // 512
    acc = None
    for j in range(tiles):
        values = jnp.concatenate([v_at[pl.ds(512 * j, 256), :], v_at[pl.ds(512 * j + 256, 256), :]], 1)
        o = jnp.dot(p_at[j], values, preferred_element_type=jnp.float32)
        acc = o if acc is None else acc + o
    row = lax.broadcasted_iota(jnp.int32, (8, 128), 0)
    for n in range(4):
        o = acc[8 * n:8 * n + 8, :128] + acc[32 + 8 * n:40 + 8 * n, 128:]
        out_at[n] = jnp.where(row < 6, o, stat_at[n])


def attend_kernel(lens_ref, q_ref, k_hbm, v_hbm, out_ref, k_buf, v_buf, p_buf, stat_buf, k_sem, v_sem):
    rows = q_ref.shape[0]
    depth = k_buf.shape[1]
    base = lax.axis_index('seq') * depth

    def k_copy(r):
        slot = lax.rem(r, SLOTS)
        return pltpu.make_async_copy(k_hbm.at[r], k_buf.at[slot], k_sem.at[slot])

    def v_copy(r):
        slot = lax.rem(r, SLOTS)
        return pltpu.make_async_copy(v_hbm.at[r], v_buf.at[slot], v_sem.at[slot])

    def prime(r, c):
        k_copy(r).start()
        v_copy(r).start()
        return c
    lax.fori_loop(0, SLOTS, prime, 0)

    def step(i, c):
        first = i * UNROLL
        parity = lax.rem(i, 2)
        for u in range(UNROLL):
            k_copy(first + u).wait()
        back = first - UNROLL
        for u in range(UNROLL):
            @pl.when(i > 0)
            def _():
                v_copy(back + u).wait()
        for u in range(UNROLL):
            limit = lens_ref[first + u] * 4 - base
            score_row(q_ref[first + u], k_buf.at[lax.rem(first + u, SLOTS)], limit,
                      p_buf.at[parity, u], stat_buf.at[parity, u])
            r = lax.max(back + u, 0)
            value_row(p_buf.at[1 - parity, u], v_buf.at[lax.rem(r, SLOTS)], stat_buf.at[1 - parity, u],
                      out_ref.at[r])
        for u in range(UNROLL):
            @pl.when(first + u + SLOTS < rows)
            def _():
                k_copy(first + u + SLOTS).start()

            @pl.when((i > 0) & (back + u + SLOTS < rows))
            def _():
                v_copy(back + u + SLOTS).start()
        return c
    steps = rows // UNROLL
    lax.fori_loop(0, steps, step, 0)
    for u in range(UNROLL):
        r = rows - UNROLL + u
        v_copy(r).wait()
        value_row(p_buf.at[(steps - 1) % 2, u], v_buf.at[r % SLOTS], stat_buf.at[(steps - 1) % 2, u], out_ref.at[r])


def attend(seq_lens, q_all, k_loc, v_loc):
    rows, depth = k_loc.shape[0], k_loc.shape[1]
    return pl.pallas_call(
        attend_kernel,
        out_shape=jax.ShapeDtypeStruct((rows, 4, 8, HEAD_DIM), jnp.float32),
        in_specs=[pl.BlockSpec(memory_space=pltpu.SMEM), pl.BlockSpec(memory_space=pltpu.VMEM),
                  pl.BlockSpec(memory_space=pl.ANY), pl.BlockSpec(memory_space=pl.ANY)],
        out_specs=pl.BlockSpec(memory_space=pltpu.VMEM),
        scratch_shapes=[
            pltpu.VMEM((SLOTS, depth, HEAD_DIM), jnp.bfloat16),
            pltpu.VMEM((SLOTS, depth, HEAD_DIM), jnp.bfloat16),
            pltpu.VMEM((2, UNROLL, depth // 512, 64, 256), jnp.bfloat16),
            pltpu.VMEM((2, UNROLL, 4, 8, HEAD_DIM), jnp.float32),
            pltpu.SemaphoreType.DMA((SLOTS,)),
            pltpu.SemaphoreType.DMA((SLOTS,)),
        ],
        compiler_params=pltpu.CompilerParams(vmem_limit_bytes=50 * 2 ** 20),
    )(seq_lens, q_all, k_loc, v_loc)


def solution(mesh):
    def local_step(x_hidden, seq_lens, k_loc, v_loc, wq_loc, wo_loc):
        rows, t_dev, kv_loc, head_dim = k_loc.shape
        q_raw = jnp.einsum('bd,dhk->bhk', x_hidden, wq_loc, preferred_element_type=jnp.float32)
        cosine, sine = rope_tables(seq_lens)
        cosine, sine = cosine[:, None, :], sine[:, None, :]
        first, second = q_raw[..., :head_dim // 2], q_raw[..., head_dim // 2:]
        q_own = jnp.concatenate([first * cosine - second * sine, second * cosine + first * sine], axis=-1).astype(jnp.bfloat16)
        q_all = lax.all_gather(q_own, 'seq', axis=1, tiled=True).reshape(rows, kv_loc, 6, head_dim)
        q_all = jnp.pad(q_all, ((0, 0), (0, 0), (0, 2), (0, 0))).reshape(rows, kv_loc * 8, head_dim)
        part = attend(seq_lens, q_all, k_loc.reshape(rows, t_dev * kv_loc, head_dim),
                      v_loc.reshape(rows, t_dev * kv_loc, head_dim))
        local_max = part[:, :, 6, :6]
        local_sum = part[:, :, 7, :6]
        global_max = lax.pmax(local_max, 'seq')
        rescale = jnp.exp2(local_max - global_max)
        out_own = lax.psum_scatter(part[:, :, :6] * rescale[..., None], 'seq', scatter_dimension=1, tiled=True)
        sum_own = lax.psum_scatter(local_sum * rescale, 'seq', scatter_dimension=1, tiled=True)
        attn = (out_own / sum_own[..., None]).astype(jnp.bfloat16).reshape(rows, 6, head_dim)
        y_part = jnp.einsum('bhk,hkd->bd', attn, wo_loc, preferred_element_type=jnp.float32)
        y_sum = lax.psum(y_part, ('kvh', 'seq'))
        return (x_hidden.astype(jnp.float32) + y_sum).astype(jnp.bfloat16)

    return jax.shard_map(
        local_step,
        mesh=mesh,
        in_specs=(P('dp', None), P('dp'), P('dp', 'seq', 'kvh', None), P('dp', 'seq', 'kvh', None),
                  P(None, ('kvh', 'seq'), None), P(('kvh', 'seq'), None, None)),
        out_specs=P('dp', None),
        check_vma=False)
```

```python
import functools

import jax
import jax.numpy as jnp
from jax import lax
from jax.experimental import pallas as pl
from jax.experimental.pallas import tpu as pltpu
from jax.sharding import PartitionSpec as P

ROPE_THETA = 500000.0
HEAD_DIM = 128
NEG = -3.3e38
FLOOR = -3.0e38
LOG2E = 1.4426950408889634
SCALE2 = HEAD_DIM ** -0.5 * LOG2E
SLOTS = 16
UNROLL = 4
Q_ROWS = 32
PART_ROWS = 16
Q_DEPTH = 512
MESH = pl.DeviceIdType.MESH


def rope_tables(seq_lens):
    half_dim = HEAD_DIM // 2
    inv_freq = jnp.power(ROPE_THETA, -jnp.arange(half_dim, dtype=jnp.float32) * (2.0 / HEAD_DIM))
    angle = (seq_lens - 1).astype(jnp.float32)[:, None] * inv_freq[None, :]
    cosine, sine = jnp.cos(angle), jnp.sin(angle)
    return jnp.concatenate([cosine, cosine], -1), jnp.concatenate([-sine, sine], -1)


def head_lanes(width):
    lane = lax.broadcasted_iota(jnp.int32, (8, width), 1)
    return lane, [lane % 4 == n for n in range(4)]


def pick(masks, parts):
    return jnp.where(masks[0], parts[0], jnp.where(masks[1], parts[1], jnp.where(masks[2], parts[2], parts[3])))


def score_row(q32, k_at, limit, s_at, top_at):
    tiles = k_at.shape[0] // 512
    zero = jnp.zeros_like(q32)
    q_diag = jnp.concatenate([jnp.concatenate([q32, zero], 1), jnp.concatenate([zero, q32], 1)], 0)
    lane, masks = head_lanes(256)
    top = None
    for j in range(tiles):
        keys = jnp.concatenate([k_at[pl.ds(512 * j, 256), :], k_at[pl.ds(512 * j + 256, 256), :]], 1)
        s = lax.dot_general(q_diag, keys, (((1,), (1,)), ((), ())), preferred_element_type=jnp.float32)
        for h in range(2):
            mine = pick(masks, [s[32 * h + 8 * n:32 * h + 8 * n + 8] for n in range(4)])
            mine = jnp.where(lane < limit - (512 * j + 256 * h), mine, NEG)
            s_at[:, pl.ds(512 * j + 256 * h, 256)] = mine
            top = mine if top is None else jnp.maximum(top, mine)
    top_at[...] = jnp.maximum(top[:, :128], top[:, 128:])


def weight_row(s_at, top_at, p_at, stat_at):
    tiles = s_at.shape[1] // 512
    _, masks = head_lanes(256)
    _, half = head_lanes(128)
    top = top_at[...]
    tops = [jnp.maximum(jnp.max(jnp.where(half[n], top, NEG), axis=1, keepdims=True), FLOOR) * SCALE2 for n in range(4)]
    shift = pick(half, tops)
    shift = jnp.concatenate([shift, shift], 1)
    total = None
    for j in range(tiles):
        rows = []
        for h in range(2):
            w = jnp.exp2(s_at[:, pl.ds(512 * j + 256 * h, 256)] * SCALE2 - shift)
            total = w if total is None else total + w
            rows += [jnp.where(masks[n], w, 0.0) for n in range(4)]
        p_at[j] = jnp.concatenate(rows, 0).astype(jnp.bfloat16)
    total = total[:, :128] + total[:, 128:]
    row = lax.broadcasted_iota(jnp.int32, (8, 128), 0)
    lane128 = lax.broadcasted_iota(jnp.int32, (8, 128), 1)
    diagonal = row == lane128
    for n in range(4):
        sums = jnp.sum(jnp.where(half[n], total, 0.0), axis=1, keepdims=True)
        top_row = jnp.sum(jnp.where(diagonal, tops[n], 0.0), axis=0, keepdims=True)
        sum_row = jnp.sum(jnp.where(diagonal, sums, 0.0), axis=0, keepdims=True)
        stat_at[n] = jnp.where(row == 6, top_row, sum_row)


def value_row(p_at, v_at, stat_at, out, r):
    tiles = v_at.shape[0] // 512
    acc = None
    for j in range(tiles):
        values = jnp.concatenate([v_at[pl.ds(512 * j, 256), :], v_at[pl.ds(512 * j + 256, 256), :]], 1)
        o = jnp.dot(p_at[j], values, preferred_element_type=jnp.float32)
        acc = o if acc is None else acc + o
    row = lax.broadcasted_iota(jnp.int32, (8, 128), 0)
    for n in range(4):
        o = acc[8 * n:8 * n + 8, :128] + acc[32 + 8 * n:40 + 8 * n, 128:]
        out[n, r] = jnp.where(row < 6, o, stat_at[n])


def add_up(parts):
    return functools.reduce(lambda a, b: a + b, parts)


def merge_rows(parts):
    maxima = [p[:, 6:7, :] for p in parts]
    top = functools.reduce(jnp.maximum, maxima)
    scale = [jnp.exp2(m - top) for m in maxima]
    total = add_up([p[:, 7:8, :] * e for p, e in zip(parts, scale)])
    shape = parts[0].shape
    diagonal = lax.broadcasted_iota(jnp.int32, shape, 1) == lax.broadcasted_iota(jnp.int32, shape, 2)
    factors = [jnp.sum(jnp.where(diagonal, jnp.broadcast_to(e / total, shape), 0.0), axis=2, keepdims=True) for e in scale]
    return add_up([p * f for p, f in zip(parts, factors)])


def decode_kernel(lens_ref, cos_ref, sin_ref, x_hbm, wq_hbm, k_hbm, v_hbm, wo_hbm, out_hbm,
                  x_buf, wq_buf, wo_buf, k_buf, v_buf, q_acc, q_rows, q_all, s_buf, top_buf, p_buf, stat_buf,
                  part, part_in, attn_rows, attn_buf, y_send, y_own, r1, r2, r3, out_buf,
                  x_sem, wq_sem, wo_sem, k_sem, v_sem, q_ssem, q_rsem, part_ssem, part_rsem,
                  y1_ssem, y1_rsem, y2_ssem, y2_rsem, y3_ssem, y3_rsem, ag_ssem, ag_rsem, out_sem):
    rows, model = x_buf.shape
    depth = k_buf.shape[1]
    width = y_own.shape[2]
    groups = rows // UNROLL
    dp, y, s = lax.axis_index('dp'), lax.axis_index('kvh'), lax.axis_index('seq')
    c, x = lax.rem(s, 2), lax.div(s, 2)
    base = s * depth
    seq_peers = [s + 1 - 2 * c, lax.rem(s + 2, 4), 3 - s]
    partner = (dp, y, s + 1 - 2 * c)
    first_axis = (dp, y + c * (1 - 2 * y), lax.rem(s + 2 * (1 - c), 4))
    second_axis = (dp, y + (1 - c) * (1 - 2 * y), lax.rem(s + 2 * c, 4))
    am, bm = x + c * (y - x), y + c * (x - y)

    def remote(src, dst, ssem, rsem, device):
        return pltpu.make_async_remote_copy(src_ref=src, dst_ref=dst, send_sem=ssem, recv_sem=rsem,
                                            device_id=device, device_id_type=MESH)

    barrier = pltpu.get_barrier_semaphore()
    for device in [(dp, y, p) for p in seq_peers] + [(dp, 1 - y, s)]:
        pl.semaphore_signal(barrier, inc=1, device_id=device, device_id_type=MESH)

    x_copy = pltpu.make_async_copy(x_hbm, x_buf, x_sem)
    x_copy.start()

    def wq_copy(i):
        return pltpu.make_async_copy(wq_hbm.at[:, pl.ds(i * Q_DEPTH, Q_DEPTH), :], wq_buf.at[i], wq_sem.at[i])

    def wo_copy(i):
        return pltpu.make_async_copy(wo_hbm.at[:, pl.ds(pl.multiple_of(i * width, 128), width)], wo_buf.at[i], wo_sem.at[i])

    def k_copy(r):
        slot = lax.rem(r, SLOTS)
        return pltpu.make_async_copy(k_hbm.at[r], k_buf.at[slot], k_sem.at[slot])

    def v_copy(r):
        slot = lax.rem(r, SLOTS)
        return pltpu.make_async_copy(v_hbm.at[r], v_buf.at[slot], v_sem.at[slot])

    def each(n, f, first=0):
        def step(i, carry):
            f(i)
            return carry
        lax.fori_loop(first, n, step, 0)

    q_steps = model // Q_DEPTH
    each(q_steps, lambda i: wq_copy(i).start())

    def prime(r):
        k_copy(r).start()
        v_copy(r).start()
    each(SLOTS, prime)
    each(8, lambda i: wo_copy(i).start())

    q_acc[...] = jnp.zeros_like(q_acc)
    q_rows[...] = jnp.zeros_like(q_rows)
    x_copy.wait()

    def project(i):
        wq_copy(i).wait()
        weights = jnp.concatenate([wq_buf[i, g] for g in range(6)], 1)
        cols = pl.ds(pl.multiple_of(i * Q_DEPTH, 128), Q_DEPTH)
        q_acc[...] += jnp.dot(x_buf[:, cols], weights, preferred_element_type=jnp.float32)
    each(q_steps, project)
    for g in range(6):
        q = q_acc[:, g * HEAD_DIM:(g + 1) * HEAD_DIM]
        q = q * cos_ref[...] + pltpu.roll(q, HEAD_DIM // 2, 1) * sin_ref[...]
        q_rows[pl.ds(g, rows, stride=8), :] = q
    q_all[s] = q_rows[...].reshape(rows, 8, HEAD_DIM).astype(jnp.bfloat16)
    pl.semaphore_wait(barrier, 4)

    def q_send(d, i):
        piece = q_all.at[s, pl.ds(i * Q_ROWS, Q_ROWS)]
        return remote(piece, piece, q_ssem.at[d, i], q_rsem.at[d, i], (dp, y, seq_peers[d]))

    def q_chunk(i):
        for d in range(3):
            q_send(d, i).start()
    each(rows // Q_ROWS, q_chunk)

    def part_send(d, i):
        chunk = pl.ds(i * PART_ROWS, PART_ROWS)
        return remote(part.at[seq_peers[d], chunk], part_in.at[d, chunk], part_ssem.at[d, i], part_rsem.at[d, i],
                      (dp, y, seq_peers[d]))

    def merge(i):
        for d in range(3):
            part_send(d, i).wait_recv()
        for h in range(PART_ROWS // 8):
            chunk = pl.ds(i * PART_ROWS + 8 * h, 8)
            merged = merge_rows([part[s, chunk]] + [part_in[d, chunk] for d in range(3)])
            attn_rows[pl.ds(pl.multiple_of((i * PART_ROWS + 8 * h) * 8, 64), 64), :] = merged.reshape(64, HEAD_DIM)

    def attend(i, stages):
        parity = lax.rem(i, 2)
        ahead = i * UNROLL
        back = (i - 2) * UNROLL
        if 'a' in stages:
            @pl.when(lax.rem(ahead, Q_ROWS) == 0)
            def _():
                for d in range(3):
                    q_send(d, lax.div(ahead, Q_ROWS)).wait_recv()
            for u in range(UNROLL):
                k_copy(ahead + u).wait()
        if 'c' in stages:
            for u in range(UNROLL):
                v_copy(back + u).wait()
        if 'a' in stages:
            for u in range(UNROLL):
                r = ahead + u
                q32 = jnp.concatenate([q_all[n, r] for n in range(4)], 0)
                score_row(q32, k_buf.at[lax.rem(r, SLOTS)], lens_ref[r] * 4 - base, s_buf.at[parity, u], top_buf.at[parity, u])
        if 'c' in stages:
            for u in range(UNROLL):
                r = back + u
                value_row(p_buf.at[parity, u], v_buf.at[lax.rem(r, SLOTS)], stat_buf.at[parity, u], part, r)
        if 'b' in stages:
            for u in range(UNROLL):
                weight_row(s_buf.at[1 - parity, u], top_buf.at[1 - parity, u], p_buf.at[1 - parity, u], stat_buf.at[1 - parity, u])
        if 'a' in stages:
            @pl.when(ahead + SLOTS < rows)
            def _():
                for u in range(UNROLL):
                    k_copy(ahead + u + SLOTS).start()
        if 'c' in stages:
            @pl.when(back + SLOTS < rows)
            def _():
                for u in range(UNROLL):
                    v_copy(back + u + SLOTS).start()

            @pl.when(lax.rem(back + UNROLL, PART_ROWS) == 0)
            def _():
                chunk = lax.div(back, PART_ROWS)
                for d in range(3):
                    part_send(d, chunk).start()

                @pl.when(chunk > 0)
                def _():
                    merge(chunk - 1)
    attend(0, 'a')
    attend(1, 'ab')
    each(groups, lambda i: attend(i, 'abc'), 2)
    attend(groups, 'bc')
    attend(groups + 1, 'c')
    merge(rows // PART_ROWS - 1)

    for g in range(6):
        attn_buf[:, g * HEAD_DIM:(g + 1) * HEAD_DIM] = attn_rows[pl.ds(g, rows, stride=8), :].astype(jnp.bfloat16)
    each(8, lambda i: wo_copy(i).wait())

    def block(b):
        return jnp.dot(attn_buf[...], wo_buf[b], preferred_element_type=jnp.float32)

    def to_partner(j):
        return remote(y_send.at[j], r1.at[j], y1_ssem.at[j], y1_rsem.at[j], partner)

    def partner_half(j):
        y_send[j] = block(4 * (1 - c) + j)
        to_partner(j).start()
    each(4, partner_half)

    def to_first(k):
        return remote(y_own.at[k], r2.at[k], y2_ssem.at[k], y2_rsem.at[k], first_axis)

    def own_half(k):
        o = 2 * ((1 - am) + lax.div(k, 2) * (2 * am - 1)) + (1 - bm) + lax.rem(k, 2) * (2 * bm - 1)
        mine = block(4 * c + o)
        to_partner(o).wait_recv()
        y_own[k] = mine + r1[o]

        @pl.when(k < 2)
        def _():
            to_first(k).start()
    each(4, own_half)

    to_first(0).wait_recv()
    y_own[2] = y_own[2] + r2[0]
    to_second = remote(y_own.at[2], r3, y3_ssem, y3_rsem, second_axis)
    to_second.start()
    to_first(1).wait_recv()
    y_own[3] = y_own[3] + r2[1]
    to_second.wait_recv()

    def block_id(fa, fb):
        a = am if fa == 0 else 1 - am
        b = bm if fb == 0 else 1 - bm
        return 4 * c + 2 * a + b
    mine = block_id(0, 0)
    x_cols = x_buf[:, pl.ds(pl.multiple_of(mine * width, 128), width)].astype(jnp.float32)
    out_buf[mine] = (x_cols + (y_own[3] + r3[...])).astype(jnp.bfloat16)

    def gather(i, b, device):
        return remote(out_buf.at[b], out_buf.at[b], ag_ssem.at[i], ag_rsem.at[i], device)

    def store(b):
        return pltpu.make_async_copy(out_buf.at[b], out_hbm.at[:, pl.ds(pl.multiple_of(b * width, 128), width)], out_sem.at[b])
    blocks = [block_id(0, 0), block_id(0, 1), block_id(1, 0), block_id(1, 1)]
    theirs = [4 - 4 * c + j for j in range(4)]
    sends = [gather(0, blocks[0], second_axis), gather(1, blocks[0], first_axis), gather(3, blocks[0], partner)]
    for send in sends:
        send.start()
    store(blocks[0]).start()

    def pass_on(i, b, targets):
        gather(i, b, partner).wait_recv()
        for j, device in targets:
            send = gather(j, b, device)
            send.start()
            sends.append(send)
        store(b).start()
    pass_on(0, blocks[1], [(2, first_axis), (4, partner)])
    pass_on(1, blocks[2], [(5, partner)])
    pass_on(2, blocks[3], [(6, partner)])
    pc = 1 - c
    pam, pbm = x + pc * (y - x), y + pc * (x - y)
    partner_blocks = [4 * pc + 2 * pam + pbm, 4 * pc + 2 * pam + 1 - pbm, 4 * pc + 2 * (1 - pam) + pbm, 4 * pc + 2 * (1 - pam) + 1 - pbm]
    for i, b in zip((3, 4, 5, 6), partner_blocks):
        gather(i, b, partner).wait_recv()
        store(b).start()

    for d in range(3):
        each(rows // Q_ROWS, lambda i: q_send(d, i).wait_send())
        each(rows // PART_ROWS, lambda i: part_send(d, i).wait_send())
    each(4, lambda j: to_partner(j).wait_send())
    each(2, lambda k: to_first(k).wait_send())
    to_second.wait_send()
    for send in sends:
        send.wait_send()
    each(8, lambda b: store(b).wait())


def decode(seq_lens, x_hidden, k_loc, v_loc, wq_loc, wo_loc):
    rows, depth = k_loc.shape[0], k_loc.shape[1]
    model = x_hidden.shape[1]
    width = model // 8
    cosine, sine = rope_tables(seq_lens)
    bf16, f32 = jnp.bfloat16, jnp.float32
    dma = pltpu.SemaphoreType.DMA
    q_chunks, part_chunks = rows // Q_ROWS, rows // PART_ROWS
    vmem, hbm = pl.BlockSpec(memory_space=pltpu.VMEM), pl.BlockSpec(memory_space=pl.ANY)
    return pl.pallas_call(
        decode_kernel,
        out_shape=jax.ShapeDtypeStruct((rows, model), bf16),
        in_specs=[pl.BlockSpec(memory_space=pltpu.SMEM), vmem, vmem, hbm, hbm, hbm, hbm, hbm],
        out_specs=hbm,
        scratch_shapes=[
            pltpu.VMEM((rows, model), bf16),
            pltpu.VMEM((model // Q_DEPTH, 6, Q_DEPTH, HEAD_DIM), bf16),
            pltpu.VMEM((8, 6 * HEAD_DIM, width), bf16),
            pltpu.VMEM((SLOTS, depth, HEAD_DIM), bf16),
            pltpu.VMEM((SLOTS, depth, HEAD_DIM), bf16),
            pltpu.VMEM((rows, 6 * HEAD_DIM), f32),
            pltpu.VMEM((rows * 8, HEAD_DIM), f32),
            pltpu.VMEM((4, rows, 8, HEAD_DIM), bf16),
            pltpu.VMEM((2, UNROLL, 8, depth), f32),
            pltpu.VMEM((2, UNROLL, 8, HEAD_DIM), f32),
            pltpu.VMEM((2, UNROLL, depth // 512, 64, 256), bf16),
            pltpu.VMEM((2, UNROLL, 4, 8, HEAD_DIM), f32),
            pltpu.VMEM((4, rows, 8, HEAD_DIM), f32),
            pltpu.VMEM((3, rows, 8, HEAD_DIM), f32),
            pltpu.VMEM((rows * 8, HEAD_DIM), f32),
            pltpu.VMEM((rows, 6 * HEAD_DIM), bf16),
            pltpu.VMEM((4, rows, width), f32),
            pltpu.VMEM((4, rows, width), f32),
            pltpu.VMEM((4, rows, width), f32),
            pltpu.VMEM((2, rows, width), f32),
            pltpu.VMEM((rows, width), f32),
            pltpu.VMEM((8, rows, width), bf16),
            dma, dma((model // Q_DEPTH,)), dma((8,)), dma((SLOTS,)), dma((SLOTS,)),
            dma((3, q_chunks)), dma((3, q_chunks)), dma((3, part_chunks)), dma((3, part_chunks)),
            dma((4,)), dma((4,)), dma((2,)), dma((2,)), dma, dma, dma((7,)), dma((7,)), dma((8,)),
        ],
        compiler_params=pltpu.CompilerParams(vmem_limit_bytes=62 * 2 ** 20, collective_id=0, has_side_effects=True),
    )(seq_lens, cosine, sine, x_hidden, wq_loc, k_loc, v_loc, wo_loc)


def solution(mesh):
    def local_step(x_hidden, seq_lens, k_loc, v_loc, wq_loc, wo_loc):
        rows, t_dev, kv_loc, head_dim = k_loc.shape
        return decode(seq_lens, x_hidden, k_loc.reshape(rows, t_dev * kv_loc, head_dim),
                      v_loc.reshape(rows, t_dev * kv_loc, head_dim), wq_loc.transpose(1, 0, 2),
                      wo_loc.reshape(-1, wo_loc.shape[2]))

    return jax.shard_map(
        local_step,
        mesh=mesh,
        in_specs=(P('dp', None), P('dp'), P('dp', 'seq', 'kvh', None), P('dp', 'seq', 'kvh', None),
                  P(None, ('kvh', 'seq'), None), P(('kvh', 'seq'), None, None)),
        out_specs=P('dp', None),
        check_vma=False)
```

```python
import functools

import jax
import jax.numpy as jnp
import numpy as np
from jax import lax
from jax.experimental import pallas as pl
from jax.experimental.pallas import tpu as pltpu
from jax.sharding import PartitionSpec as P

ROPE_THETA = 500000.0
HEAD_DIM = 128
NEG = -3.3e38
FLOOR = -3.0e38
LOG2E = 1.4426950408889634
SCALE2 = HEAD_DIM ** -0.5 * LOG2E
SLOTS = 16
UNROLL = 4
Q_ROWS = 32
PART_ROWS = 8
PART_LAG = 2
ROW_GROUPS = ((0, 48), (48, 48), (96, 32))
Q_DEPTH = 512
LOOP_STEPS = ((17, 0, 'project'), (19, 0, 'first'), (23, 0, 'second'), (27, 0, 'finish'), (29, 1, 'project'), (31, 1, 'first'))
TAIL_STEPS = ((2, 'project'), (0, 'relay'), (1, 'second'), (2, 'first'), (0, 'relay_last'), (1, 'finish'), (2, 'second'), (2, 'finish'),
              (1, 'relay'), (1, 'relay_last'), (0, 'collect'), (2, 'relay'), (2, 'relay_last'), (1, 'collect'), (2, 'collect'))
MESH = pl.DeviceIdType.MESH


def head_lanes(width):
    lane = lax.broadcasted_iota(jnp.int32, (8, width), 1)
    return lane, [lane % 4 == n for n in range(4)]


def pick(masks, parts):
    return jnp.where(masks[0], parts[0], jnp.where(masks[1], parts[1], jnp.where(masks[2], parts[2], parts[3])))


def score_row(q32, k_at, limit, s_at, top_at):
    tiles = k_at.shape[0] // 512
    zero = jnp.zeros_like(q32)
    q_diag = jnp.concatenate([jnp.concatenate([q32, zero], 1), jnp.concatenate([zero, q32], 1)], 0)
    lane, masks = head_lanes(256)
    top = None
    for j in range(tiles):
        keys = jnp.concatenate([k_at[pl.ds(512 * j, 256), :], k_at[pl.ds(512 * j + 256, 256), :]], 1)
        s = lax.dot_general(q_diag, keys, (((1,), (1,)), ((), ())), preferred_element_type=jnp.float32)
        for h in range(2):
            mine = pick(masks, [s[32 * h + 8 * n:32 * h + 8 * n + 8] for n in range(4)])
            mine = jnp.where(lane < limit - (512 * j + 256 * h), mine, NEG)
            s_at[:, pl.ds(512 * j + 256 * h, 256)] = mine
            top = mine if top is None else jnp.maximum(top, mine)
    top_at[...] = jnp.maximum(top[:, :128], top[:, 128:])


def weight_row(s_at, top_at, p_at, stat_at):
    tiles = s_at.shape[1] // 512
    _, masks = head_lanes(256)
    _, half = head_lanes(128)
    top = top_at[...]
    tops = [jnp.maximum(jnp.max(jnp.where(half[n], top, NEG), axis=1, keepdims=True), FLOOR) * SCALE2 for n in range(4)]
    shift = pick(half, tops)
    shift = jnp.concatenate([shift, shift], 1)
    total = None
    for j in range(tiles):
        rows = []
        for h in range(2):
            w = jnp.exp2(s_at[:, pl.ds(512 * j + 256 * h, 256)] * SCALE2 - shift)
            total = w if total is None else total + w
            rows += [jnp.where(masks[n], w, 0.0) for n in range(4)]
        p_at[j] = jnp.concatenate(rows, 0).astype(jnp.bfloat16)
    total = total[:, :128] + total[:, 128:]
    row = lax.broadcasted_iota(jnp.int32, (8, 128), 0)
    lane128 = lax.broadcasted_iota(jnp.int32, (8, 128), 1)
    diagonal = row == lane128
    for n in range(4):
        sums = jnp.sum(jnp.where(half[n], total, 0.0), axis=1, keepdims=True)
        top_row = jnp.sum(jnp.where(diagonal, tops[n], 0.0), axis=0, keepdims=True)
        sum_row = jnp.sum(jnp.where(diagonal, sums, 0.0), axis=0, keepdims=True)
        stat_at[n] = jnp.where(row == 6, top_row, sum_row)


def value_row(p_at, v_at, stat_at, out, r):
    tiles = v_at.shape[0] // 512
    acc = None
    for j in range(tiles):
        values = jnp.concatenate([v_at[pl.ds(512 * j, 256), :], v_at[pl.ds(512 * j + 256, 256), :]], 1)
        o = jnp.dot(p_at[j], values, preferred_element_type=jnp.float32)
        acc = o if acc is None else acc + o
    row = lax.broadcasted_iota(jnp.int32, (8, 128), 0)
    for n in range(4):
        o = acc[8 * n:8 * n + 8, :128] + acc[32 + 8 * n:40 + 8 * n, 128:]
        out[n, r] = jnp.where(row < 6, o, stat_at[n])


def add_up(parts):
    return functools.reduce(lambda a, b: a + b, parts)


def merge_rows(parts):
    maxima = [p[:, 6:7, :] for p in parts]
    top = functools.reduce(jnp.maximum, maxima)
    scale = [jnp.exp2(m - top) for m in maxima]
    total = add_up([p[:, 7:8, :] * e for p, e in zip(parts, scale)])
    shape = parts[0].shape
    diagonal = lax.broadcasted_iota(jnp.int32, shape, 1) == lax.broadcasted_iota(jnp.int32, shape, 2)
    factors = [jnp.sum(jnp.where(diagonal, jnp.broadcast_to(e / total, shape), 0.0), axis=2, keepdims=True) for e in scale]
    return add_up([p * f for p, f in zip(parts, factors)])


def decode_kernel(lens_ref, freq_hbm, x_hbm, wq_hbm, k_hbm, v_hbm, wo_hbm, out_hbm,
                  freq_buf, pos_buf, cos_buf, sin_buf, x_buf, wq_buf, wo_buf, k_buf, v_buf, q_acc, q_rows, q_all, s_buf, top_buf, p_buf, stat_buf,
                  part, part_in, attn_rows, attn_buf, y_send, y_own, r1, r2, r3, out_buf,
                  freq_sem, x_sem, wq_sem, wo_sem, k_sem, v_sem, q_ssem, q_rsem, part_ssem, part_rsem,
                  y1_ssem, y1_rsem, y2_ssem, y2_rsem, y3_ssem, y3_rsem, ag_ssem, ag_rsem, out_sem):
    rows, model = x_buf.shape
    depth = k_buf.shape[1]
    width = y_own.shape[2]
    groups = rows // UNROLL
    dp, y, s = lax.axis_index('dp'), lax.axis_index('kvh'), lax.axis_index('seq')
    c, x = lax.rem(s, 2), lax.div(s, 2)
    base = s * depth
    seq_peers = [s + 1 - 2 * c, lax.rem(s + 2, 4), 3 - s]
    partner = (dp, y, s + 1 - 2 * c)

    def remote(src, dst, ssem, rsem, device):
        return pltpu.make_async_remote_copy(src_ref=src, dst_ref=dst, send_sem=ssem, recv_sem=rsem,
                                            device_id=device, device_id_type=MESH)

    barrier = pltpu.get_barrier_semaphore()
    for device in [(dp, y, p) for p in seq_peers] + [(dp, 1 - y, s)]:
        pl.semaphore_signal(barrier, inc=1, device_id=device, device_id_type=MESH)

    freq_copy = pltpu.make_async_copy(freq_hbm, freq_buf, freq_sem)
    freq_copy.start()
    x_copy = pltpu.make_async_copy(x_hbm, x_buf, x_sem)
    x_copy.start()

    def wq_copy(i):
        return pltpu.make_async_copy(wq_hbm.at[:, pl.ds(i * Q_DEPTH, Q_DEPTH), :], wq_buf.at[i], wq_sem.at[i])

    def wo_copy(i):
        return pltpu.make_async_copy(wo_hbm.at[:, pl.ds(pl.multiple_of(i * width, 128), width)], wo_buf.at[i], wo_sem.at[i])

    def k_copy(r):
        slot = lax.rem(r, SLOTS)
        return pltpu.make_async_copy(k_hbm.at[r], k_buf.at[slot], k_sem.at[slot])

    def v_copy(r):
        slot = lax.rem(r, SLOTS)
        return pltpu.make_async_copy(v_hbm.at[r], v_buf.at[slot], v_sem.at[slot])

    def each(n, f, first=0):
        def step(i, carry):
            f(i)
            return carry
        lax.fori_loop(first, n, step, 0)

    q_steps = model // Q_DEPTH
    each(q_steps, lambda i: wq_copy(i).start())

    def prime(r):
        k_copy(r).start()
        v_copy(r).start()
    each(SLOTS, prime)
    each(8, lambda i: wo_copy(i).start())

    q_acc[...] = jnp.zeros_like(q_acc)
    q_rows[...] = jnp.zeros_like(q_rows)

    def position(i):
        for u in range(8):
            r = 8 * i + u
            pos_buf[pl.ds(r, 1), :] = jnp.broadcast_to(lens_ref[r] - 1, (1, HEAD_DIM)).astype(jnp.float32)
    each(rows // 8, position)
    freq_copy.wait()
    angle = pos_buf[...] * freq_buf[...]
    q_sin = jnp.sin(angle)
    lane = lax.broadcasted_iota(jnp.int32, angle.shape, 1)
    cos_buf[...] = jnp.cos(angle)
    sin_buf[...] = jnp.where(lane < HEAD_DIM // 2, -q_sin, q_sin)
    x_copy.wait()

    def project(i):
        wq_copy(i).wait()
        weights = jnp.concatenate([wq_buf[i, g] for g in range(6)], 1)
        cols = pl.ds(pl.multiple_of(i * Q_DEPTH, 128), Q_DEPTH)
        q_acc[...] += jnp.dot(x_buf[:, cols], weights, preferred_element_type=jnp.float32)
    each(q_steps, project)
    for g in range(6):
        q = q_acc[:, g * HEAD_DIM:(g + 1) * HEAD_DIM]
        q = q * cos_buf[...] + pltpu.roll(q, HEAD_DIM // 2, 1) * sin_buf[...]
        q_rows[pl.ds(g, rows, stride=8), :] = q
    q_all[s] = q_rows[...].reshape(rows, 8, HEAD_DIM).astype(jnp.bfloat16)
    pl.semaphore_wait(barrier, 4)

    def q_send(d, i):
        piece = q_all.at[s, pl.ds(i * Q_ROWS, Q_ROWS)]
        return remote(piece, piece, q_ssem.at[d, i], q_rsem.at[d, i], (dp, y, seq_peers[d]))

    def q_chunk(i):
        for d in range(3):
            q_send(d, i).start()
    each(rows // Q_ROWS, q_chunk)

    def part_send(d, i):
        chunk = pl.ds(i * PART_ROWS, PART_ROWS)
        return remote(part.at[seq_peers[d], chunk], part_in.at[d, chunk], part_ssem.at[d, i], part_rsem.at[d, i],
                      (dp, y, seq_peers[d]))

    def merge(i):
        for d in range(3):
            part_send(d, i).wait_recv()
        chunk = pl.ds(i * PART_ROWS, PART_ROWS)
        merged = merge_rows([part[s, chunk]] + [part_in[d, chunk] for d in range(3)])
        span = PART_ROWS * 8
        attn_rows[pl.ds(pl.multiple_of(i * span, span), span), :] = merged.reshape(span, HEAD_DIM)

    def attend(i, stages):
        parity = lax.rem(i, 2)
        ahead = i * UNROLL
        back = (i - 2) * UNROLL
        if 'a' in stages:
            @pl.when(lax.rem(ahead, Q_ROWS) == 0)
            def _():
                for d in range(3):
                    q_send(d, lax.div(ahead, Q_ROWS)).wait_recv()
            for u in range(UNROLL):
                k_copy(ahead + u).wait()
        if 'c' in stages:
            for u in range(UNROLL):
                v_copy(back + u).wait()
        if 'a' in stages:
            for u in range(UNROLL):
                r = ahead + u
                q32 = jnp.concatenate([q_all[n, r] for n in range(4)], 0)
                score_row(q32, k_buf.at[lax.rem(r, SLOTS)], lens_ref[r] * 4 - base, s_buf.at[parity, u], top_buf.at[parity, u])
        if 'c' in stages:
            for u in range(UNROLL):
                r = back + u
                value_row(p_buf.at[parity, u], v_buf.at[lax.rem(r, SLOTS)], stat_buf.at[parity, u], part, r)
        if 'b' in stages:
            for u in range(UNROLL):
                weight_row(s_buf.at[1 - parity, u], top_buf.at[1 - parity, u], p_buf.at[1 - parity, u], stat_buf.at[1 - parity, u])
        if 'a' in stages:
            @pl.when(ahead + SLOTS < rows)
            def _():
                for u in range(UNROLL):
                    k_copy(ahead + u + SLOTS).start()
        if 'c' in stages:
            @pl.when(back + SLOTS < rows)
            def _():
                for u in range(UNROLL):
                    v_copy(back + u + SLOTS).start()

            @pl.when(lax.rem(back + UNROLL, PART_ROWS) == 0)
            def _():
                chunk = lax.div(back, PART_ROWS)
                for d in range(3):
                    part_send(d, chunk).start()

                @pl.when(chunk >= PART_LAG)
                def _():
                    merge(chunk - PART_LAG)

    def reduction(g, first_row, count, early):
        span = pl.ds(first_row, count)
        cc = 1 if early else c
        first_axis = (dp, y + cc * (1 - 2 * y), lax.rem(s + 2 * (1 - cc), 4))
        second_axis = (dp, y + (1 - cc) * (1 - 2 * y), lax.rem(s + 2 * cc, 4))
        am, bm = x + cc * (y - x), y + cc * (x - y)
        sends = []

        def block(b):
            return jnp.dot(attn_buf[span, :], wo_buf[b], preferred_element_type=jnp.float32)

        def to_partner(j):
            return remote(y_send.at[j, span], r1.at[j, span], y1_ssem.at[g, j], y1_rsem.at[g, j], partner)

        def offset(k):
            fa, fb = 1 - k // 2, 1 - k % 2
            return 2 * (am + fa * (1 - 2 * am)) + bm + fb * (1 - 2 * bm)

        def to_first(k):
            return remote(y_own.at[k, span], r2.at[k, span], y2_ssem.at[g, k], y2_rsem.at[g, k], first_axis)

        def to_second():
            return remote(y_own.at[2, span], r3.at[span], y3_ssem.at[g], y3_rsem.at[g], second_axis)

        def gather(i, b, device):
            return remote(out_buf.at[b, span], out_buf.at[b, span], ag_ssem.at[g, i], ag_rsem.at[g, i], device)

        def store(b):
            return pltpu.make_async_copy(out_buf.at[b, span], out_hbm.at[span, pl.ds(pl.multiple_of(b * width, 128), width)],
                                         out_sem.at[g, b])
        blocks = [4 * c + offset(3 - i) for i in range(4)]

        def project():
            for h in range(6):
                rows_of_head = attn_rows[pl.ds(8 * first_row + h, count, stride=8), :]
                attn_buf[span, h * HEAD_DIM:(h + 1) * HEAD_DIM] = rows_of_head.astype(jnp.bfloat16)

            def partner_half(j):
                ahead = [block(4 * (1 - c) + 2 * j + u) for u in range(2)]
                for u in range(2):
                    y_send[2 * j + u, span, :] = ahead[u]
                    to_partner(2 * j + u).start()
            each(2, partner_half)

            def own_half(k):
                fa = 1 - k
                base_block = 4 * c + 2 * (am + fa * (1 - 2 * am))
                ahead = [block(base_block + bm + (1 - u) * (1 - 2 * bm)) for u in range(2)]
                for u in range(2):
                    y_own[2 * k + u, span, :] = ahead[u]
            each(2, own_half)

        def first():
            for k in range(4):
                o = offset(k)
                to_partner(o).wait_recv()
                y_own[k, span, :] = y_own[k, span, :] + r1[o, span, :]
                if k < 2:
                    to_first(k).start()

        def second():
            to_first(0).wait_recv()
            y_own[2, span, :] = y_own[2, span, :] + r2[0, span, :]
            to_second().start()

        def finish():
            to_first(1).wait_recv()
            y_own[3, span, :] = y_own[3, span, :] + r2[1, span, :]
            to_second().wait_recv()
            x_cols = x_buf[span, pl.ds(pl.multiple_of(blocks[0] * width, 128), width)].astype(jnp.float32)
            out_buf[blocks[0], span, :] = (x_cols + (y_own[3, span, :] + r3[span, :])).astype(jnp.bfloat16)
            for i, device in ((0, second_axis), (1, first_axis), (3, partner)):
                sends.append(gather(i, blocks[0], device))
                sends[-1].start()
            store(blocks[0]).start()

        def pass_on(i, targets):
            b = blocks[1 + i]
            gather(i, b, partner).wait_recv()
            for j, device in targets:
                sends.append(gather(j, b, device))
                sends[-1].start()
            store(b).start()

        def relay():
            pass_on(0, [(2, first_axis), (4, partner)])
            pass_on(1, [(5, partner)])

        def relay_last():
            pass_on(2, [(6, partner)])

        def collect():
            pc = 1 - c
            pcc = 1 if early else pc
            pam, pbm = x + pcc * (y - x), y + pcc * (x - y)
            for i in range(4):
                a = pam if i < 2 else 1 - pam
                b = 4 * pc + 2 * a + (pbm if i % 2 == 0 else 1 - pbm)
                gather(3 + i, b, partner).wait_recv()
                store(b).start()

        def drain():
            each(4, lambda j: to_partner(j).wait_send())
            each(2, lambda k: to_first(k).wait_send())
            to_second().wait_send()
            for send in sends:
                send.wait_send()
            each(8, lambda b: store(b).wait())
        return dict(project=project, first=first, second=second, finish=finish, relay=relay, relay_last=relay_last,
                    collect=collect, drain=drain)
    reductions = [reduction(g, r, n, g + 1 < len(ROW_GROUPS)) for g, (r, n) in enumerate(ROW_GROUPS)]

    attend(0, 'a')
    attend(1, 'ab')
    at = 2
    for stop, g, name in LOOP_STEPS:
        if stop + 1 > at:
            each(stop + 1, lambda i: attend(i, 'abc'), at)
            at = stop + 1
        if (g, name) == (0, 'project'):
            each(8, lambda i: wo_copy(i).wait())
        reductions[g][name]()
    each(groups, lambda i: attend(i, 'abc'), at)
    attend(groups, 'bc')
    attend(groups + 1, 'c')
    for i in range(PART_LAG):
        merge(rows // PART_ROWS - PART_LAG + i)
    for g, name in TAIL_STEPS:
        reductions[g][name]()

    for d in range(3):
        each(rows // Q_ROWS, lambda i: q_send(d, i).wait_send())
        each(rows // PART_ROWS, lambda i: part_send(d, i).wait_send())
    for r in reductions:
        r['drain']()


def decode(seq_lens, x_hidden, k_loc, v_loc, wq_loc, wo_loc):
    rows, depth = k_loc.shape[0], k_loc.shape[1]
    model = x_hidden.shape[1]
    width = model // 8
    inv_freq = np.power(ROPE_THETA, -np.arange(HEAD_DIM // 2) * (2.0 / HEAD_DIM)).astype(np.float32)
    inv_freq = jnp.asarray(np.concatenate([inv_freq, inv_freq])[None])
    bf16, f32 = jnp.bfloat16, jnp.float32
    dma = pltpu.SemaphoreType.DMA
    q_chunks, part_chunks = rows // Q_ROWS, rows // PART_ROWS
    n = len(ROW_GROUPS)
    hbm = pl.BlockSpec(memory_space=pl.ANY)
    return pl.pallas_call(
        decode_kernel,
        out_shape=jax.ShapeDtypeStruct((rows, model), bf16),
        in_specs=[pl.BlockSpec(memory_space=pltpu.SMEM), hbm, hbm, hbm, hbm, hbm, hbm],
        out_specs=hbm,
        scratch_shapes=[
            pltpu.VMEM((1, HEAD_DIM), f32),
            pltpu.VMEM((rows, HEAD_DIM), f32),
            pltpu.VMEM((rows, HEAD_DIM), f32),
            pltpu.VMEM((rows, HEAD_DIM), f32),
            pltpu.VMEM((rows, model), bf16),
            pltpu.VMEM((model // Q_DEPTH, 6, Q_DEPTH, HEAD_DIM), bf16),
            pltpu.VMEM((8, 6 * HEAD_DIM, width), bf16),
            pltpu.VMEM((SLOTS, depth, HEAD_DIM), bf16),
            pltpu.VMEM((SLOTS, depth, HEAD_DIM), bf16),
            pltpu.VMEM((rows, 6 * HEAD_DIM), f32),
            pltpu.VMEM((rows * 8, HEAD_DIM), f32),
            pltpu.VMEM((4, rows, 8, HEAD_DIM), bf16),
            pltpu.VMEM((2, UNROLL, 8, depth), f32),
            pltpu.VMEM((2, UNROLL, 8, HEAD_DIM), f32),
            pltpu.VMEM((2, UNROLL, depth // 512, 64, 256), bf16),
            pltpu.VMEM((2, UNROLL, 4, 8, HEAD_DIM), f32),
            pltpu.VMEM((4, rows, 8, HEAD_DIM), f32),
            pltpu.VMEM((3, rows, 8, HEAD_DIM), f32),
            pltpu.VMEM((rows * 8, HEAD_DIM), f32),
            pltpu.VMEM((rows, 6 * HEAD_DIM), bf16),
            pltpu.VMEM((4, rows, width), f32),
            pltpu.VMEM((4, rows, width), f32),
            pltpu.VMEM((4, rows, width), f32),
            pltpu.VMEM((2, rows, width), f32),
            pltpu.VMEM((rows, width), f32),
            pltpu.VMEM((8, rows, width), bf16),
            dma, dma, dma((model // Q_DEPTH,)), dma((8,)), dma((SLOTS,)), dma((SLOTS,)),
            dma((3, q_chunks)), dma((3, q_chunks)), dma((3, part_chunks)), dma((3, part_chunks)),
            dma((n, 4)), dma((n, 4)), dma((n, 2)), dma((n, 2)), dma((n,)), dma((n,)), dma((n, 7)), dma((n, 7)), dma((n, 8)),
        ],
        compiler_params=pltpu.CompilerParams(vmem_limit_bytes=62 * 2 ** 20, collective_id=0, has_side_effects=True),
    )(seq_lens, inv_freq, x_hidden, wq_loc, k_loc, v_loc, wo_loc)


def solution(mesh):
    def local_step(x_hidden, seq_lens, k_loc, v_loc, wq_loc, wo_loc):
        rows, t_dev, kv_loc, head_dim = k_loc.shape
        return decode(seq_lens, x_hidden, k_loc.reshape(rows, t_dev * kv_loc, head_dim),
                      v_loc.reshape(rows, t_dev * kv_loc, head_dim), wq_loc.transpose(1, 0, 2),
                      wo_loc.reshape(-1, wo_loc.shape[2]))

    return jax.shard_map(
        local_step,
        mesh=mesh,
        in_specs=(P('dp', None), P('dp'), P('dp', 'seq', 'kvh', None), P('dp', 'seq', 'kvh', None),
                  P(None, ('kvh', 'seq'), None), P(('kvh', 'seq'), None, None)),
        out_specs=P('dp', None),
        check_vma=False)
```

```python
import functools

import jax
import jax.numpy as jnp
import numpy as np
from jax import lax
from jax.experimental import pallas as pl
from jax.experimental.pallas import tpu as pltpu
from jax.sharding import PartitionSpec as P

ROPE_THETA = 500000.0
HEAD_DIM = 128
NEG = -3.3e38
FLOOR = -3.0e38
LOG2E = 1.4426950408889634
SCALE2 = HEAD_DIM ** -0.5 * LOG2E
SLOTS = 16
UNROLL = 4
Q_ROWS = 8
PART_ROWS = 8
PART_LAG = 2
ROW_GROUPS = ((0, 48), (48, 48), (96, 16), (112, 16))
Q_DEPTH = 512
LOOP_STEPS = ((17, 0, 'project'), (18, 0, 'first'), (23, 0, 'second'), (27, 0, 'finish'), (29, 1, 'project'), (31, 1, 'first'),
              (31, 0, 'relay'))
TAIL_STEPS = ((2, 'project'), (1, 'second'), (2, 'first'), (3, 'merge'), (3, 'project'), (3, 'first'), (2, 'second'), (0, 'relay_last'),
              (1, 'finish'), (3, 'second'), (2, 'finish'), (1, 'relay'), (3, 'finish'), (2, 'relay'), (1, 'relay_last'), (0, 'collect'),
              (3, 'relay'), (2, 'relay_last'), (1, 'collect'), (3, 'relay_last'), (2, 'collect'), (3, 'collect'))
MESH = pl.DeviceIdType.MESH


def head_lanes(width):
    lane = lax.broadcasted_iota(jnp.int32, (8, width), 1)
    return lane, [lane % 4 == n for n in range(4)]


def pick(masks, parts):
    return jnp.where(masks[0], parts[0], jnp.where(masks[1], parts[1], jnp.where(masks[2], parts[2], parts[3])))


def score_row(q32, k_at, limit, s_at, top_at):
    tiles = k_at.shape[0] // 512
    zero = jnp.zeros_like(q32)
    q_diag = jnp.concatenate([jnp.concatenate([q32, zero], 1), jnp.concatenate([zero, q32], 1)], 0)
    lane, masks = head_lanes(256)
    top = None
    for j in range(tiles):
        keys = jnp.concatenate([k_at[pl.ds(512 * j, 256), :], k_at[pl.ds(512 * j + 256, 256), :]], 1)
        s = lax.dot_general(q_diag, keys, (((1,), (1,)), ((), ())), preferred_element_type=jnp.float32)
        for h in range(2):
            mine = pick(masks, [s[32 * h + 8 * n:32 * h + 8 * n + 8] for n in range(4)])
            mine = jnp.where(lane < limit - (512 * j + 256 * h), mine, NEG)
            s_at[:, pl.ds(512 * j + 256 * h, 256)] = mine
            top = mine if top is None else jnp.maximum(top, mine)
    top_at[...] = jnp.maximum(top[:, :128], top[:, 128:])


def weight_row(s_at, top_at, p_at, stat_at):
    tiles = s_at.shape[1] // 512
    _, masks = head_lanes(256)
    _, half = head_lanes(128)
    top = top_at[...]
    tops = [jnp.maximum(jnp.max(jnp.where(half[n], top, NEG), axis=1, keepdims=True), FLOOR) * SCALE2 for n in range(4)]
    shift = pick(half, tops)
    shift = jnp.concatenate([shift, shift], 1)
    total = None
    for j in range(tiles):
        rows = []
        for h in range(2):
            w = jnp.exp2(s_at[:, pl.ds(512 * j + 256 * h, 256)] * SCALE2 - shift)
            total = w if total is None else total + w
            rows += [jnp.where(masks[n], w, 0.0) for n in range(4)]
        p_at[j] = jnp.concatenate(rows, 0).astype(jnp.bfloat16)
    total = total[:, :128] + total[:, 128:]
    row = lax.broadcasted_iota(jnp.int32, (8, 128), 0)
    lane128 = lax.broadcasted_iota(jnp.int32, (8, 128), 1)
    diagonal = row == lane128
    for n in range(4):
        sums = jnp.sum(jnp.where(half[n], total, 0.0), axis=1, keepdims=True)
        top_row = jnp.sum(jnp.where(diagonal, tops[n], 0.0), axis=0, keepdims=True)
        sum_row = jnp.sum(jnp.where(diagonal, sums, 0.0), axis=0, keepdims=True)
        stat_at[n] = jnp.where(row == 6, top_row, sum_row)


def value_row(p_at, v_at, stat_at, out, r):
    tiles = v_at.shape[0] // 512
    acc = None
    for j in range(tiles):
        values = jnp.concatenate([v_at[pl.ds(512 * j, 256), :], v_at[pl.ds(512 * j + 256, 256), :]], 1)
        o = jnp.dot(p_at[j], values, preferred_element_type=jnp.float32)
        acc = o if acc is None else acc + o
    row = lax.broadcasted_iota(jnp.int32, (8, 128), 0)
    for n in range(4):
        o = acc[8 * n:8 * n + 8, :128] + acc[32 + 8 * n:40 + 8 * n, 128:]
        out[n, r] = jnp.where(row < 6, o, stat_at[n])


def add_up(parts):
    return functools.reduce(lambda a, b: a + b, parts)


def merge_rows(parts):
    maxima = [p[:, 6:7, :] for p in parts]
    top = functools.reduce(jnp.maximum, maxima)
    scale = [jnp.exp2(m - top) for m in maxima]
    total = add_up([p[:, 7:8, :] * e for p, e in zip(parts, scale)])
    shape = parts[0].shape
    diagonal = lax.broadcasted_iota(jnp.int32, shape, 1) == lax.broadcasted_iota(jnp.int32, shape, 2)
    factors = [jnp.sum(jnp.where(diagonal, jnp.broadcast_to(e / total, shape), 0.0), axis=2, keepdims=True) for e in scale]
    return add_up([p * f for p, f in zip(parts, factors)])


def decode_kernel(lens_ref, freq_hbm, x_hbm, wq_hbm, k_hbm, v_hbm, wo_hbm, out_hbm,
                  freq_buf, pos_buf, cos_buf, sin_buf, x_buf, wq_buf, wo_buf, k_buf, v_buf, q_acc, q_rows, q_all, s_buf, top_buf, p_buf, stat_buf,
                  part, part_in, attn_rows, attn_buf, y_send, y_own, r1, r2, r3, out_buf,
                  freq_sem, x_sem, wq_sem, wo_sem, k_sem, v_sem, q_ssem, q_rsem, part_ssem, part_rsem,
                  y1_ssem, y1_rsem, y2_ssem, y2_rsem, y3_ssem, y3_rsem, ag_ssem, ag_rsem, out_sem):
    rows, model = x_buf.shape
    depth = k_buf.shape[1]
    width = y_own.shape[2]
    groups = rows // UNROLL
    dp, y, s = lax.axis_index('dp'), lax.axis_index('kvh'), lax.axis_index('seq')
    c, x = lax.rem(s, 2), lax.div(s, 2)
    base = s * depth
    seq_peers = [s + 1 - 2 * c, lax.rem(s + 2, 4), 3 - s]
    partner = (dp, y, s + 1 - 2 * c)

    def remote(src, dst, ssem, rsem, device):
        return pltpu.make_async_remote_copy(src_ref=src, dst_ref=dst, send_sem=ssem, recv_sem=rsem,
                                            device_id=device, device_id_type=MESH)

    barrier = pltpu.get_barrier_semaphore()
    for device in [(dp, y, p) for p in seq_peers] + [(dp, 1 - y, s)]:
        pl.semaphore_signal(barrier, inc=1, device_id=device, device_id_type=MESH)

    freq_copy = pltpu.make_async_copy(freq_hbm, freq_buf, freq_sem)
    freq_copy.start()
    x_copy = pltpu.make_async_copy(x_hbm, x_buf, x_sem)
    x_copy.start()

    def wq_copy(i):
        return pltpu.make_async_copy(wq_hbm.at[:, pl.ds(i * Q_DEPTH, Q_DEPTH), :], wq_buf.at[i], wq_sem.at[i])

    def wo_copy(i):
        return pltpu.make_async_copy(wo_hbm.at[:, pl.ds(pl.multiple_of(i * width, 128), width)], wo_buf.at[i], wo_sem.at[i])

    def k_copy(r):
        slot = lax.rem(r, SLOTS)
        return pltpu.make_async_copy(k_hbm.at[r], k_buf.at[slot], k_sem.at[slot])

    def v_copy(r):
        slot = lax.rem(r, SLOTS)
        return pltpu.make_async_copy(v_hbm.at[r], v_buf.at[slot], v_sem.at[slot])

    def each(n, f, first=0):
        def step(i, carry):
            f(i)
            return carry
        lax.fori_loop(first, n, step, 0)

    q_steps = model // Q_DEPTH
    each(q_steps, lambda i: wq_copy(i).start())

    def prime(r):
        k_copy(r).start()
        v_copy(r).start()
    each(SLOTS, prime)
    each(8, lambda i: wo_copy(i).start())

    q_acc[...] = jnp.zeros_like(q_acc)
    q_rows[...] = jnp.zeros_like(q_rows)

    def position(i):
        for u in range(8):
            r = 8 * i + u
            pos_buf[pl.ds(r, 1), :] = jnp.broadcast_to(lens_ref[r] - 1, (1, HEAD_DIM)).astype(jnp.float32)
    each(rows // 8, position)
    freq_copy.wait()
    angle = pos_buf[...] * freq_buf[...]
    q_sin = jnp.sin(angle)
    lane = lax.broadcasted_iota(jnp.int32, angle.shape, 1)
    cos_buf[...] = jnp.cos(angle)
    sin_buf[...] = jnp.where(lane < HEAD_DIM // 2, -q_sin, q_sin)
    with jax.named_scope('xwait'):
        x_copy.wait()

    def project(i):
        wq_copy(i).wait()
        weights = jnp.concatenate([wq_buf[i, g] for g in range(6)], 1)
        cols = pl.ds(pl.multiple_of(i * Q_DEPTH, 128), Q_DEPTH)
        q_acc[...] += jnp.dot(x_buf[:, cols], weights, preferred_element_type=jnp.float32)
    with jax.named_scope('qproj'):
        each(q_steps, project)
    for g in range(6):
        q = q_acc[:, g * HEAD_DIM:(g + 1) * HEAD_DIM]
        q = q * cos_buf[...] + pltpu.roll(q, HEAD_DIM // 2, 1) * sin_buf[...]
        q_rows[pl.ds(g, rows, stride=8), :] = q
    q_all[s] = q_rows[...].reshape(rows, 8, HEAD_DIM).astype(jnp.bfloat16)
    with jax.named_scope('barrier'):
        pl.semaphore_wait(barrier, 4)

    def q_send(d, i):
        piece = q_all.at[s, pl.ds(i * Q_ROWS, Q_ROWS)]
        return remote(piece, piece, q_ssem.at[d, i], q_rsem.at[d, i], (dp, y, seq_peers[d]))

    def q_chunk(i):
        for d in range(3):
            q_send(d, i).start()
    each(rows // Q_ROWS, q_chunk)

    def part_send(d, i):
        chunk = pl.ds(i * PART_ROWS, PART_ROWS)
        return remote(part.at[seq_peers[d], chunk], part_in.at[d, chunk], part_ssem.at[d, i], part_rsem.at[d, i],
                      (dp, y, seq_peers[d]))

    def merge(i):
        for d in range(3):
            part_send(d, i).wait_recv()
        chunk = pl.ds(i * PART_ROWS, PART_ROWS)
        merged = merge_rows([part[s, chunk]] + [part_in[d, chunk] for d in range(3)])
        span = PART_ROWS * 8
        attn_rows[pl.ds(pl.multiple_of(i * span, span), span), :] = merged.reshape(span, HEAD_DIM)

    def attend(i, stages):
        parity = lax.rem(i, 2)
        ahead = i * UNROLL
        back = (i - 2) * UNROLL
        if 'a' in stages:
            @pl.when(lax.rem(ahead, Q_ROWS) == 0)
            def _():
                for d in range(3):
                    q_send(d, lax.div(ahead, Q_ROWS)).wait_recv()
            for u in range(UNROLL):
                k_copy(ahead + u).wait()
        if 'c' in stages:
            for u in range(UNROLL):
                v_copy(back + u).wait()
        if 'a' in stages:
            for u in range(UNROLL):
                r = ahead + u
                q32 = jnp.concatenate([q_all[n, r] for n in range(4)], 0)
                score_row(q32, k_buf.at[lax.rem(r, SLOTS)], lens_ref[r] * 4 - base, s_buf.at[parity, u], top_buf.at[parity, u])
        if 'c' in stages:
            for u in range(UNROLL):
                r = back + u
                value_row(p_buf.at[parity, u], v_buf.at[lax.rem(r, SLOTS)], stat_buf.at[parity, u], part, r)
        if 'b' in stages:
            for u in range(UNROLL):
                weight_row(s_buf.at[1 - parity, u], top_buf.at[1 - parity, u], p_buf.at[1 - parity, u], stat_buf.at[1 - parity, u])
        if 'a' in stages:
            @pl.when(ahead + SLOTS < rows)
            def _():
                for u in range(UNROLL):
                    k_copy(ahead + u + SLOTS).start()
        if 'c' in stages:
            @pl.when(back + SLOTS < rows)
            def _():
                for u in range(UNROLL):
                    v_copy(back + u + SLOTS).start()

            @pl.when(lax.rem(back + UNROLL, PART_ROWS) == 0)
            def _():
                chunk = lax.div(back, PART_ROWS)
                for d in range(3):
                    part_send(d, chunk).start()

                @pl.when(chunk >= PART_LAG)
                def _():
                    merge(chunk - PART_LAG)

    def reduction(g, first_row, count, early):
        span = pl.ds(first_row, count)
        cc = 1 if early else c
        first_axis = (dp, y + cc * (1 - 2 * y), lax.rem(s + 2 * (1 - cc), 4))
        second_axis = (dp, y + (1 - cc) * (1 - 2 * y), lax.rem(s + 2 * cc, 4))
        am, bm = x + cc * (y - x), y + cc * (x - y)
        sends = []

        def block(b):
            return jnp.dot(attn_buf[span, :], wo_buf[b], preferred_element_type=jnp.float32)

        def to_partner(j):
            return remote(y_send.at[j, span], r1.at[j, span], y1_ssem.at[g, j], y1_rsem.at[g, j], partner)

        def offset(k):
            fa, fb = 1 - k // 2, 1 - k % 2
            return 2 * (am + fa * (1 - 2 * am)) + bm + fb * (1 - 2 * bm)

        def to_first(k):
            return remote(y_own.at[k, span], r2.at[k, span], y2_ssem.at[g, k], y2_rsem.at[g, k], first_axis)

        def to_second():
            return remote(y_own.at[2, span], r3.at[span], y3_ssem.at[g], y3_rsem.at[g], second_axis)

        def gather(i, b, device):
            return remote(out_buf.at[b, span], out_buf.at[b, span], ag_ssem.at[g, i], ag_rsem.at[g, i], device)

        def store(b):
            return pltpu.make_async_copy(out_buf.at[b, span], out_hbm.at[span, pl.ds(pl.multiple_of(b * width, 128), width)],
                                         out_sem.at[g, b])
        blocks = [4 * c + offset(3 - i) for i in range(4)]

        def project():
            for h in range(6):
                rows_of_head = attn_rows[pl.ds(8 * first_row + h, count, stride=8), :]
                attn_buf[span, h * HEAD_DIM:(h + 1) * HEAD_DIM] = rows_of_head.astype(jnp.bfloat16)

            def partner_half(j):
                ahead = [block(4 * (1 - c) + 2 * j + u) for u in range(2)]
                for u in range(2):
                    y_send[2 * j + u, span, :] = ahead[u]
                    to_partner(2 * j + u).start()
            each(2, partner_half)

            def own_half(k):
                fa = 1 - k
                base_block = 4 * c + 2 * (am + fa * (1 - 2 * am))
                ahead = [block(base_block + bm + (1 - u) * (1 - 2 * bm)) for u in range(2)]
                for u in range(2):
                    y_own[2 * k + u, span, :] = ahead[u]
            each(2, own_half)

        def first():
            for k in range(4):
                o = offset(k)
                to_partner(o).wait_recv()
                y_own[k, span, :] = y_own[k, span, :] + r1[o, span, :]
                if k < 2:
                    to_first(k).start()

        def second():
            to_first(0).wait_recv()
            y_own[2, span, :] = y_own[2, span, :] + r2[0, span, :]
            to_second().start()

        def finish():
            to_first(1).wait_recv()
            y_own[3, span, :] = y_own[3, span, :] + r2[1, span, :]
            to_second().wait_recv()
            x_cols = x_buf[span, pl.ds(pl.multiple_of(blocks[0] * width, 128), width)].astype(jnp.float32)
            out_buf[blocks[0], span, :] = (x_cols + (y_own[3, span, :] + r3[span, :])).astype(jnp.bfloat16)
            for i, device in ((0, second_axis), (1, first_axis), (3, partner)):
                sends.append(gather(i, blocks[0], device))
                sends[-1].start()
            store(blocks[0]).start()

        def pass_on(i, targets):
            b = blocks[1 + i]
            gather(i, b, partner).wait_recv()
            for j, device in targets:
                sends.append(gather(j, b, device))
                sends[-1].start()
            store(b).start()

        def relay():
            pass_on(0, [(2, first_axis), (4, partner)])
            pass_on(1, [(5, partner)])

        def relay_last():
            pass_on(2, [(6, partner)])

        def collect():
            pc = 1 - c
            pcc = 1 if early else pc
            pam, pbm = x + pcc * (y - x), y + pcc * (x - y)
            for i in range(4):
                a = pam if i < 2 else 1 - pam
                b = 4 * pc + 2 * a + (pbm if i % 2 == 0 else 1 - pbm)
                gather(3 + i, b, partner).wait_recv()
                store(b).start()

        def drain():
            each(4, lambda j: to_partner(j).wait_send())
            each(2, lambda k: to_first(k).wait_send())
            to_second().wait_send()
            for send in sends:
                send.wait_send()
            each(8, lambda b: store(b).wait())
        return dict(project=project, first=first, second=second, finish=finish, relay=relay, relay_last=relay_last,
                    collect=collect, drain=drain)
    reductions = [reduction(g, r, n, g + 1 < len(ROW_GROUPS)) for g, (r, n) in enumerate(ROW_GROUPS)]

    with jax.named_scope('att0'):
        attend(0, 'a')
    with jax.named_scope('att1'):
        attend(1, 'ab')
    at = 2
    for stop, g, name in LOOP_STEPS:
        if stop + 1 > at:
            with jax.named_scope(f'seg_{at}_{stop}'):
                each(stop + 1, lambda i: attend(i, 'abc'), at)
            at = stop + 1
        if g == 0 and name == 'project':
            each(8, lambda i: wo_copy(i).wait())
        with jax.named_scope(f'{name}_{g}'):
            reductions[g][name]()
    with jax.named_scope(f'seg_{at}_end'):
        each(groups, lambda i: attend(i, 'abc'), at)
    with jax.named_scope('attz'):
        attend(groups, 'bc')
    with jax.named_scope('attzz'):
        attend(groups + 1, 'c')
    def merge_last():
        for i in range(PART_LAG):
            merge(rows // PART_ROWS - PART_LAG + i)
    reductions[-1]['merge'] = merge_last
    for g, name in TAIL_STEPS:
        with jax.named_scope(f'{name}_{g}'):
            reductions[g][name]()

    for d in range(3):
        each(rows // Q_ROWS, lambda i: q_send(d, i).wait_send())
        each(rows // PART_ROWS, lambda i: part_send(d, i).wait_send())
    with jax.named_scope('drain'):
        for r in reductions:
            r['drain']()


def decode(seq_lens, x_hidden, k_loc, v_loc, wq_loc, wo_loc):
    rows, depth = k_loc.shape[0], k_loc.shape[1]
    model = x_hidden.shape[1]
    width = model // 8
    inv_freq = np.power(ROPE_THETA, -np.arange(HEAD_DIM // 2) * (2.0 / HEAD_DIM)).astype(np.float32)
    inv_freq = jnp.asarray(np.concatenate([inv_freq, inv_freq])[None])
    bf16, f32 = jnp.bfloat16, jnp.float32
    dma = pltpu.SemaphoreType.DMA
    q_chunks, part_chunks = rows // Q_ROWS, rows // PART_ROWS
    n = len(ROW_GROUPS)
    hbm = pl.BlockSpec(memory_space=pl.ANY)
    return pl.pallas_call(
        decode_kernel,
        out_shape=jax.ShapeDtypeStruct((rows, model), bf16),
        in_specs=[pl.BlockSpec(memory_space=pltpu.SMEM), hbm, hbm, hbm, hbm, hbm, hbm],
        out_specs=hbm,
        scratch_shapes=[
            pltpu.VMEM((1, HEAD_DIM), f32),
            pltpu.VMEM((rows, HEAD_DIM), f32),
            pltpu.VMEM((rows, HEAD_DIM), f32),
            pltpu.VMEM((rows, HEAD_DIM), f32),
            pltpu.VMEM((rows, model), bf16),
            pltpu.VMEM((model // Q_DEPTH, 6, Q_DEPTH, HEAD_DIM), bf16),
            pltpu.VMEM((8, 6 * HEAD_DIM, width), bf16),
            pltpu.VMEM((SLOTS, depth, HEAD_DIM), bf16),
            pltpu.VMEM((SLOTS, depth, HEAD_DIM), bf16),
            pltpu.VMEM((rows, 6 * HEAD_DIM), f32),
            pltpu.VMEM((rows * 8, HEAD_DIM), f32),
            pltpu.VMEM((4, rows, 8, HEAD_DIM), bf16),
            pltpu.VMEM((2, UNROLL, 8, depth), f32),
            pltpu.VMEM((2, UNROLL, 8, HEAD_DIM), f32),
            pltpu.VMEM((2, UNROLL, depth // 512, 64, 256), bf16),
            pltpu.VMEM((2, UNROLL, 4, 8, HEAD_DIM), f32),
            pltpu.VMEM((4, rows, 8, HEAD_DIM), f32),
            pltpu.VMEM((3, rows, 8, HEAD_DIM), f32),
            pltpu.VMEM((rows * 8, HEAD_DIM), f32),
            pltpu.VMEM((rows, 6 * HEAD_DIM), bf16),
            pltpu.VMEM((4, rows, width), f32),
            pltpu.VMEM((4, rows, width), f32),
            pltpu.VMEM((4, rows, width), f32),
            pltpu.VMEM((2, rows, width), f32),
            pltpu.VMEM((rows, width), f32),
            pltpu.VMEM((8, rows, width), bf16),
            dma, dma, dma((model // Q_DEPTH,)), dma((8,)), dma((SLOTS,)), dma((SLOTS,)),
            dma((3, q_chunks)), dma((3, q_chunks)), dma((3, part_chunks)), dma((3, part_chunks)),
            dma((n, 4)), dma((n, 4)), dma((n, 2)), dma((n, 2)), dma((n,)), dma((n,)), dma((n, 7)), dma((n, 7)), dma((n, 8)),
        ],
        compiler_params=pltpu.CompilerParams(vmem_limit_bytes=62 * 2 ** 20, collective_id=0, has_side_effects=True),
    )(seq_lens, inv_freq, x_hidden, wq_loc, k_loc, v_loc, wo_loc)


def solution(mesh):
    def local_step(x_hidden, seq_lens, k_loc, v_loc, wq_loc, wo_loc):
        rows, t_dev, kv_loc, head_dim = k_loc.shape
        return decode(seq_lens, x_hidden, k_loc.reshape(rows, t_dev * kv_loc, head_dim),
                      v_loc.reshape(rows, t_dev * kv_loc, head_dim), wq_loc.transpose(1, 0, 2),
                      wo_loc.reshape(-1, wo_loc.shape[2]))

    return jax.shard_map(
        local_step,
        mesh=mesh,
        in_specs=(P('dp', None), P('dp'), P('dp', 'seq', 'kvh', None), P('dp', 'seq', 'kvh', None),
                  P(None, ('kvh', 'seq'), None), P(('kvh', 'seq'), None, None)),
        out_specs=P('dp', None),
        check_vma=False)
```
